32 devices in a mesh: dp: 8 (over z, x), tensor: 4 (over y, core).
Axes of the slice: x: 2, y: 2, z: 4, core: 2. Of those that a mesh axis runs over, the one named last changes fastest.
Arguments:
- hidden_in: bfloat16 [32, 128, 4096], P(('dp', 'tensor')), parts along dimension 0, may hold values from -6 to 6
- norm_gain: float32 [4096], replicated, may hold values from 0.1 to 1.9
- query_weight: bfloat16 [4096, 4096], P(None, 'tensor'), may hold values from -3 to 3
- kv_weight: bfloat16 [4096, 2048], P(None, 'tensor'), may hold values from -3 to 3
- output_weight: bfloat16 [4096, 4096], P('tensor'), may hold values from -0.09375 to 0.09375
Outputs:
- attention_out: bfloat16 [32, 128, 4096], P(('dp', 'tensor')), parts along dimension 0
The draws below stay inside these ranges and needn't reach their ends.
There are 8 independent parts, one for each index of `dp`. The reference program is written for one: setup_inputs(seed, part) draws one part's arguments, and reference() takes and returns one part's arrays. A program takes and returns all parts, laid end to end along the dimension named above; an argument that names none is the same for every part. Nothing has to cross between parts.
All inputs are finite; a program needn't handle non-finite values.
Results may differ from the reference program's by a relative error of at most 0.014.
The reference program's roundings to bfloat16 on the way (of `normed`, `probabilities` and `mixed`) count: a program that leaves them out, or rounds other values in their place, can miss the bound.
Values may be sent and summed in bfloat16 or wider, within the bound.
No kernel may reach another device: no remote copies, remote signals or barrier semaphores. Data moves between devices by JAX's collectives and lax.ppermute only.
A program may use at most 128 MiB of HBM per device.

```python
import math
import jax
import jax.numpy as jnp
from jax import lax

D = 4096
H = 32
KVH = 8
HD = 128
SEQ_LEN = 128
SEQS = 4


def projection_base(key):
    base = jnp.clip(jax.random.normal(jax.random.fold_in(key, 11), (D, H * HD), jnp.float32), -4.0, 4.0)
    return base


def draw_query_weight(key, part):
    base = projection_base(key)
    return (base * D ** (-0.5)).astype(jnp.bfloat16)


def draw_kv_weight(key, part):
    own_part = jnp.clip(jax.random.normal(jax.random.fold_in(key, 13), (D, KVH * HD), jnp.float32), -4.0, 4.0)
    value_part = jnp.clip(jax.random.normal(jax.random.fold_in(key, 14), (D, KVH * HD), jnp.float32), -4.0, 4.0)
    key_part = own_part
    joined = jnp.stack((key_part.reshape(D, KVH, HD), value_part.reshape(D, KVH, HD)), axis=2)
    return (joined.reshape(D, 2 * KVH * HD) * D ** (-0.5)).astype(jnp.bfloat16)


def block_levels(key, shape, cuts, smallest, largest):
    gain = 1.0
    for axis_at, blocks in cuts:
        heights = jax.random.uniform(jax.random.fold_in(jax.random.fold_in(key, 6), axis_at), (blocks,), jnp.float32, smallest / len(cuts), largest / len(cuts))
        gain = gain * jnp.repeat(jnp.exp(heights), shape[axis_at] // blocks).reshape((-1,) + (1,) * (len(shape) - 1 - axis_at))
    return gain


def noise(rng, dims, spread, most, shards=(), held_as=jnp.bfloat16):
    values = spread * jax.random.normal(rng, dims, jnp.float32)
    if shards:
        values = values * block_levels(rng, dims, shards, -0.22, 0.18)
    return jnp.clip(values, -most, most).astype(held_as)


def setup_inputs(seed: int = 0, part: int = 0) -> dict:
    seeds = jax.random.split(jax.random.key(seed), 6)
    own_keys = jax.random.split(jax.random.fold_in(seeds[5], part), 6)
    hidden_in = noise(own_keys[0], (SEQS, SEQ_LEN, D), 1.0, 6.0, ((0, 4),))
    norm_gain = jnp.clip(1.0 + 0.18 * jax.random.normal(seeds[1], (D,), jnp.float32), 0.1, 1.9)
    query_weight = draw_query_weight(jax.random.fold_in(seeds[5], 71), part)
    kv_weight = draw_kv_weight(jax.random.fold_in(seeds[5], 71), part)
    output_weight = noise(seeds[4], (H * HD, D), (H * HD) ** -0.5, 0.09375, ((0, 4),))
    return {"hidden_in": hidden_in, "norm_gain": norm_gain, "query_weight": query_weight, "kv_weight": kv_weight, "output_weight": output_weight}


EPS = 1e-05
THETA = 500000.0

def rotary(tensor, positions):
    half_width = tensor.shape[-1] // 2
    frequency = THETA ** (-(jnp.arange(half_width, dtype=jnp.float32) * 2.0 / tensor.shape[-1]))
    angles = positions[:, None] * frequency[None, :]
    cosine = jnp.cos(angles)[:, None, :]
    sine_part = jnp.sin(angles)[:, None, :]
    first_half = tensor[..., :half_width]
    second_half = tensor[..., half_width:]
    return jnp.concatenate((first_half * cosine - second_half * sine_part, second_half * cosine + first_half * sine_part), axis=-1)

def rms_norm(hidden_in, norm_gain):
    wide = hidden_in.astype(jnp.float32)
    mean_square = lax.optimization_barrier(jnp.mean(wide * wide, axis=-1, keepdims=True))
    return (wide * lax.rsqrt(mean_square + EPS) * norm_gain).astype(jnp.bfloat16)

def attend(queries, keys, values):
    length = queries.shape[1]
    scores = jnp.einsum('bqhgd,bkhd->bhgqk', queries.astype(jnp.float32), keys.astype(jnp.float32)) / math.sqrt(queries.shape[-1])
    causal = jnp.arange(length)[:, None] >= jnp.arange(length)[None, :]
    scores = jnp.where(causal, scores, -1e+30)
    highest = lax.optimization_barrier(jnp.max(scores, axis=-1, keepdims=True))
    exponent = jnp.exp(scores - highest)
    probabilities = (exponent / lax.optimization_barrier(jnp.sum(exponent, axis=-1, keepdims=True))).astype(jnp.bfloat16)
    mixed = jnp.einsum('bhgqk,bkhd->bqhgd', probabilities.astype(jnp.float32), values.astype(jnp.float32))
    return mixed.astype(jnp.bfloat16)

def reference(hidden_in, norm_gain, query_weight, kv_weight, output_weight):
    normed = rms_norm(hidden_in, norm_gain).astype(jnp.float32)
    queries_raw = jnp.einsum('bld,dc->blc', normed, query_weight.astype(jnp.float32))
    kv_raw = jnp.einsum('bld,dc->blc', normed, kv_weight.astype(jnp.float32)).astype(jnp.bfloat16)
    kv_split = kv_raw.reshape(SEQS, SEQ_LEN, KVH, 2, HD)
    keys_raw = kv_split[:, :, :, 0, :]
    values = kv_split[:, :, :, 1, :]
    positions = jnp.arange(SEQ_LEN, dtype=jnp.float32)
    queries = rotary(queries_raw.reshape(SEQS, SEQ_LEN, H, HD), positions).astype(jnp.bfloat16)
    keys_wide = lax.optimization_barrier(keys_raw).astype(jnp.float32)
    keys = rotary(keys_wide, positions).astype(jnp.bfloat16)
    mixed = attend(queries.reshape(SEQS, SEQ_LEN, KVH, H // KVH, HD), keys, values)
    result = jnp.einsum('blc,cd->bld', mixed.reshape(SEQS, SEQ_LEN, H * HD).astype(jnp.float32), output_weight.astype(jnp.float32))
    return result.astype(jnp.bfloat16)
```

```python
import functools
import math

import jax
import jax.numpy as jnp
from jax import lax
from jax.experimental import pallas as pl
from jax.experimental.pallas import tpu as pltpu
from jax.sharding import PartitionSpec as P


KVH = 8
HD = 128

EPS = 1e-05
THETA = 500000.0

CHUNKS = 2
K_STEPS = 2
OUT_STEPS = 4


def hop(value, bit):
    pairs = [(source, source ^ bit) for source in range(lax.axis_size("tensor"))]
    return lax.ppermute(value, "tensor", pairs)


def rotary_tables(length):
    half_width = HD // 2
    frequency = THETA ** (-(jnp.arange(half_width, dtype=jnp.float32) * 2.0 / HD))
    angles = jnp.arange(length, dtype=jnp.float32)[:, None] * frequency[None, :]
    cosine = jnp.cos(angles)
    sine = jnp.sin(angles)
    return (
        jnp.concatenate((cosine, cosine), axis=1),
        jnp.concatenate((-sine, sine), axis=1),
    )


def block_kernel(*refs, pieces, has_past, first, k_steps, kv_heads, group):
    hidden = refs[:pieces]
    gain, wq, wkv, wo, cosine_ref, sine_ref = refs[pieces : pieces + 6]
    at = pieces + 6
    past = refs[at] if has_past else None
    at += has_past
    outs = refs[at : at + pieces]
    kv_out, normed, q_acc, kv_acc, mixed_all = refs[at + pieces :]
    step = pl.program_id(0)
    k_at = step % k_steps
    head = step // k_steps
    seqs, tokens, width = hidden[0].shape
    rows = seqs * tokens
    k_block = width // k_steps

    @pl.when(step == 0)
    def _():
        for piece, ref in enumerate(hidden):
            for seq in range(seqs):
                wide = ref[seq].astype(jnp.float32)
                mean_square = jnp.mean(wide * wide, axis=-1, keepdims=True)
                result = (wide * lax.rsqrt(mean_square + EPS) * gain[...]).astype(jnp.bfloat16)
                base = piece * rows + seq * tokens
                for k in range(k_steps):
                    normed[k, base : base + tokens, :] = result[:, k * k_block : (k + 1) * k_block]

    @pl.when(step < kv_heads * k_steps)
    def _():
        x = normed[k_at]
        q_part = jnp.dot(x, wq[...], preferred_element_type=jnp.float32)
        kv_part = jnp.dot(x, wkv[...], preferred_element_type=jnp.float32)

        @pl.when(k_at == 0)
        def _():
            q_acc[...] = q_part
            kv_acc[...] = kv_part

        @pl.when(k_at > 0)
        def _():
            q_acc[...] += q_part
            kv_acc[...] += kv_part

    @pl.when((step < kv_heads * k_steps) & (k_at == k_steps - 1))
    def _():
        cosine = cosine_ref[...]
        sine = sine_ref[...]

        def rotate(value):
            return (value * cosine + pltpu.roll(value, HD // 2, 1) * sine).astype(jnp.bfloat16)

        scale = 1.0 / math.sqrt(HD)
        total = first + tokens
        query_at = lax.broadcasted_iota(jnp.int32, (group * tokens, total), 0) % tokens + first
        key_at = lax.broadcasted_iota(jnp.int32, (group * tokens, total), 1)
        causal = query_at >= key_at
        for seq in range(pieces * seqs):
            span = slice(seq * tokens, (seq + 1) * tokens)
            queries = jnp.concatenate(
                [rotate(q_acc[span, h * HD : (h + 1) * HD]) for h in range(group)], axis=0
            )
            raw = kv_acc[span, :].astype(jnp.bfloat16)
            keys = rotate(raw[:, :HD].astype(jnp.float32))
            values = raw[:, HD:]
            kv_out[seq, :, :HD] = keys
            kv_out[seq, :, HD:] = values
            if has_past:
                keys = jnp.concatenate((past[seq, :, :HD], keys), axis=0)
                values = jnp.concatenate((past[seq, :, HD:], values), axis=0)
            scores = lax.dot_general(
                queries, keys, (((1,), (1,)), ((), ())), preferred_element_type=jnp.float32
            )
            scores = jnp.where(causal, scores * scale, -1e30)
            highest = jnp.max(scores, axis=-1, keepdims=True)
            exponent = jnp.exp(scores - highest)
            total_weight = jnp.sum(exponent, axis=-1, keepdims=True)
            probabilities = (exponent / total_weight).astype(jnp.bfloat16)
            mixed = jnp.dot(probabilities, values, preferred_element_type=jnp.float32)
            mixed = mixed.astype(jnp.bfloat16)
            for h in range(group):
                mixed_all[head, span, h * HD : (h + 1) * HD] = mixed[
                    h * tokens : (h + 1) * tokens, :
                ]

    @pl.when(step >= kv_heads * k_steps)
    def _():
        joined = jnp.concatenate([mixed_all[h] for h in range(kv_heads)], axis=1)
        out = jnp.dot(joined, wo[...], preferred_element_type=jnp.float32)
        for piece, ref in enumerate(outs):
            for seq in range(seqs):
                base = piece * rows + seq * tokens
                ref[seq] = out[base : base + tokens].astype(ref.dtype)


def block(hidden, weights, tables, past, first):
    gain, wq, wkv, wo = weights
    pieces = len(hidden)
    seqs, tokens, width = hidden[0].shape
    rows = pieces * seqs * tokens
    kv_heads = wkv.shape[1] // (2 * HD)
    group = wq.shape[1] // HD // kv_heads
    k_block = width // K_STEPS
    attend_steps = kv_heads * K_STEPS
    out_block = wo.shape[1] // OUT_STEPS
    cosine, sine = (table[first : first + tokens] for table in tables)

    def whole(shape):
        return pl.BlockSpec(shape, lambda s: (0,) * len(shape))

    def weight_at(s):
        held = jnp.minimum(s, attend_steps - 1)
        return held % K_STEPS, held // K_STEPS

    def out_at(s):
        return jnp.maximum(s - attend_steps, 0)

    in_specs = [whole((seqs, tokens, width)) for _ in hidden] + [
        whole((1, width)),
        pl.BlockSpec((k_block, group * HD), weight_at),
        pl.BlockSpec((k_block, 2 * HD), weight_at),
        pl.BlockSpec((wo.shape[0], out_block), lambda s: (0, out_at(s))),
        whole((tokens, HD)),
        whole((tokens, HD)),
    ]
    operands = [*hidden, gain, wq, wkv, wo, cosine, sine]
    if past is not None:
        in_specs.append(
            pl.BlockSpec((pieces * seqs, first, 2 * HD), lambda s: (0, 0, weight_at(s)[1]))
        )
        operands.append(past)
    kernel = functools.partial(
        block_kernel,
        pieces=pieces,
        has_past=past is not None,
        first=first,
        k_steps=K_STEPS,
        kv_heads=kv_heads,
        group=group,
    )
    flops = 2 * rows * width * (wq.shape[1] + wkv.shape[1] + wo.shape[0])
    result = pl.pallas_call(
        kernel,
        grid=(attend_steps + OUT_STEPS,),
        in_specs=in_specs,
        out_specs=[
            pl.BlockSpec((seqs, tokens, out_block), lambda s: (0, 0, out_at(s))) for _ in hidden
        ]
        + [pl.BlockSpec((pieces * seqs, tokens, 2 * HD), lambda s: (0, 0, weight_at(s)[1]))],
        out_shape=[
            jax.ShapeDtypeStruct(
                (seqs, tokens, wo.shape[1]), jnp.bfloat16 if piece % 2 else jnp.float32
            )
            for piece in range(pieces)
        ]
        + [jax.ShapeDtypeStruct((pieces * seqs, tokens, wkv.shape[1]), jnp.bfloat16)],
        scratch_shapes=[
            pltpu.VMEM((K_STEPS, rows, k_block), jnp.bfloat16),
            pltpu.VMEM((rows, group * HD), jnp.float32),
            pltpu.VMEM((rows, 2 * HD), jnp.float32),
            pltpu.VMEM((kv_heads, rows, group * HD), jnp.bfloat16),
        ],
        compiler_params=pltpu.CompilerParams(
            dimension_semantics=("arbitrary",), vmem_limit_bytes=44 * 2**20
        ),
        cost_estimate=pl.CostEstimate(
            flops=flops,
            transcendentals=0,
            bytes_accessed=2 * (wq.size + wkv.size + wo.size),
        ),
    )(*operands)
    return result[:-1], result[-1]


def finish_kernel(*refs):
    *addends, _, out = refs
    total = addends[0][...]
    for ref in addends[1:]:
        total = total + ref[...].astype(jnp.float32)
    out[...] = total.astype(jnp.bfloat16)


def finish(own, whole_came, came, previous, c, chunk):
    seqs, _, width = own.shape
    column = width // 2
    ranged = pl.BlockSpec((seqs, chunk, column), lambda i: (0, c, i))
    single = pl.BlockSpec((seqs, chunk, column), lambda i: (0, 0, i))
    addends = [own, *whole_came, *came]
    specs = [ranged] * (1 + len(whole_came)) + [single] * len(came)
    aliases = {}
    if previous is None:
        previous = jnp.zeros((8, 128), jnp.bfloat16)
    else:
        aliases = {len(addends): 0}
    return pl.pallas_call(
        finish_kernel,
        grid=(width // column,),
        in_specs=specs + [pl.BlockSpec(memory_space=pl.ANY)],
        out_specs=ranged,
        out_shape=jax.ShapeDtypeStruct(own.shape, jnp.bfloat16),
        input_output_aliases=aliases,
        compiler_params=pltpu.CompilerParams(
            dimension_semantics=("arbitrary",), vmem_limit_bytes=16 * 2**20
        ),
    )(*addends, previous)


def join_heads(kv_weight):
    sharers = max(lax.axis_size("tensor") // KVH, 1)
    position = lax.axis_index("tensor")
    for bit_index in range(sharers.bit_length() - 1):
        bit = 1 << bit_index
        partner = hop(kv_weight, bit)
        keeps_first = position // bit % 2 == 0
        kv_weight = jnp.concatenate(
            (
                jnp.where(keeps_first, kv_weight, partner),
                jnp.where(keeps_first, partner, kv_weight),
            ),
            axis=1,
        )
    return kv_weight


def layer(hidden_in, norm_gain, query_weight, kv_weight, output_weight):
    parts = lax.axis_size("tensor")
    _, length, width = hidden_in.shape
    tables = rotary_tables(length)
    weights = (norm_gain.reshape(1, width), query_weight, join_heads(kv_weight), output_weight)
    near = [m for m in range(parts) if m < 2]
    far = [m for m in range(parts) if m >= 2]
    groups = [far[i : i + 2] for i in range(0, len(far), 2)]
    chunk = length // CHUNKS
    spans = [slice(c * chunk, (c + 1) * chunk) for c in range(CHUNKS)]

    arrived = {0: hidden_in}
    if len(near) > 1:
        arrived[1] = hop(hidden_in, 1)
    far_arrived = []
    for span in spans:
        held = {0: hidden_in[:, span]}
        for m in far:
            low = m & -m
            if m ^ low == 1:
                held[1] = arrived[1][:, span]
            held[m] = hop(held[m ^ low], low)
        far_arrived.append(held)

    near_out, _ = block([arrived[m] for m in near], weights, tables, None, 0)
    own = near_out[0]
    near_came = []
    if len(near) > 1:
        near_came = [hop(near_out[1], 1)]

    pasts = [None for _ in groups]
    result = None
    for c in range(CHUNKS):
        totals = {}
        for g, group in enumerate(groups):
            out, kv = block(
                [far_arrived[c][m] for m in group], weights, tables, pasts[g], c * chunk
            )
            pasts[g] = kv if pasts[g] is None else jnp.concatenate((pasts[g], kv), axis=1)
            totals.update(zip(group, out))
        came = []
        for m in reversed(far):
            low = m & -m
            back = hop(totals[m].astype(jnp.bfloat16), low)
            if m ^ low:
                totals[m ^ low] = totals[m ^ low] + back.astype(jnp.float32)
            else:
                came.append(back)
        result = finish(own, near_came, came, result, c, chunk)
    return result


def solution(mesh):
    placed = (
        P(("dp", "tensor"), None, None),
        P(),
        P(None, "tensor"),
        P(None, "tensor"),
        P("tensor", None),
    )
    return jax.shard_map(
        layer,
        mesh=mesh,
        in_specs=placed,
        out_specs=P(("dp", "tensor"), None, None),
        check_vma=False,
    )
```

```python
import functools
import math

import jax
import jax.numpy as jnp
from jax import lax
from jax.experimental import pallas as pl
from jax.experimental.pallas import tpu as pltpu
from jax.sharding import PartitionSpec as P


KVH = 8
HD = 128

EPS = 1e-05
THETA = 500000.0

CHUNKS = 2
K_STEPS = 2
OUT_STEPS = 4
VMEM_LIMIT = 12 * 2**20


def hop(value, bit):
    pairs = [(source, source ^ bit) for source in range(lax.axis_size("tensor"))]
    return lax.ppermute(value, "tensor", pairs)


def rotary_tables(length):
    half_width = HD // 2
    frequency = THETA ** (-(jnp.arange(half_width, dtype=jnp.float32) * 2.0 / HD))
    angles = jnp.arange(length, dtype=jnp.float32)[:, None] * frequency[None, :]
    cosine = jnp.cos(angles)
    sine = jnp.sin(angles)
    return (
        jnp.concatenate((cosine, cosine), axis=1),
        jnp.concatenate((-sine, sine), axis=1),
    )


def block_kernel(*refs, pieces, load, has_past, first, kv_heads, group):
    hidden = list(refs[:pieces])
    gain, wq, wkv, wo, cosine_ref, sine_ref = refs[pieces : pieces + 6]
    at = pieces + 6
    past = refs[at] if has_past else None
    at += has_past
    outs = refs[at : at + pieces]
    at += pieces
    copies = {}
    if load:
        wq_to, wkv_to, wo_to, normed, q_acc, kv_acc, mixed_all, held, gain_to, sems = refs[at:]
        k_steps = K_STEPS
    else:
        kv_out, normed, q_acc, kv_acc, mixed_all = refs[at:]
        k_steps = 1
    seqs, tokens, width = hidden[0].shape
    rows = seqs * tokens
    k_block = width // k_steps
    out_block = wo.shape[1] // OUT_STEPS

    def k_span(k):
        return slice(k * k_block, (k + 1) * k_block)

    def q_span(head):
        return slice(head * group * HD, (head + 1) * group * HD)

    def kv_span(head):
        return slice(head * 2 * HD, (head + 1) * 2 * HD)

    def out_span(n):
        return slice(n * out_block, (n + 1) * out_block)

    if load:

        def start(name, source, target):
            copy = pltpu.make_async_copy(source, target, sems.at[len(copies)])
            copy.start()
            copies[name] = copy

        start("gain", gain, gain_to)
        for piece, ref in enumerate(hidden):
            start(("x", piece), ref, held.at[piece])
            hidden[piece] = held.at[piece]
        for head in range(kv_heads):
            for k in range(k_steps):
                source = (k_span(k), q_span(head))
                start(("q", head, k), wq.at[source], wq_to.at[source])
                source = (k_span(k), kv_span(head))
                start(("kv", head, k), wkv.at[source], wkv_to.at[source])
        for n in range(OUT_STEPS):
            source = (slice(None), out_span(n))
            start(("o", n), wo.at[source], wo_to.at[source])
        gain, wq, wkv, wo = gain_to, wq_to, wkv_to, wo_to

    def ready(*name):
        if load:
            copies[name if len(name) > 1 else name[0]].wait()

    ready("gain")
    for piece, ref in enumerate(hidden):
        ready("x", piece)
        for seq in range(seqs):
            wide = ref[seq].astype(jnp.float32)
            mean_square = jnp.mean(wide * wide, axis=-1, keepdims=True)
            result = (wide * lax.rsqrt(mean_square + EPS) * gain[...]).astype(jnp.bfloat16)
            base = piece * rows + seq * tokens
            normed[base : base + tokens, :] = result

    cosine = cosine_ref[...]
    sine = sine_ref[...]

    def rotate(value):
        return (value * cosine + pltpu.roll(value, HD // 2, 1) * sine).astype(jnp.bfloat16)

    scale = 1.0 / math.sqrt(HD)
    total = first + tokens
    query_at = lax.broadcasted_iota(jnp.int32, (tokens, total), 0) + first
    key_at = lax.broadcasted_iota(jnp.int32, (tokens, total), 1)
    causal = jnp.concatenate([query_at - key_at] * group, axis=0) >= 0

    for head in range(kv_heads):
        for k in range(k_steps):
            ready("q", head, k)
            ready("kv", head, k)
            x = normed[:, k_span(k)]
            q_part = jnp.dot(x, wq[k_span(k), q_span(head)], preferred_element_type=jnp.float32)
            kv_part = jnp.dot(x, wkv[k_span(k), kv_span(head)], preferred_element_type=jnp.float32)
            if k == 0:
                q_acc[head] = q_part
                kv_acc[head] = kv_part
            else:
                q_acc[head] += q_part
                kv_acc[head] += kv_part
        for seq in range(pieces * seqs):
            span = slice(seq * tokens, (seq + 1) * tokens)
            queries = jnp.concatenate(
                [rotate(q_acc[head, span, h * HD : (h + 1) * HD]) for h in range(group)], axis=0
            )
            raw = kv_acc[head, span, :].astype(jnp.bfloat16)
            keys = rotate(raw[:, :HD].astype(jnp.float32))
            values = raw[:, HD:]
            if not load:
                kv_out[seq, :, head * 2 * HD : (head * 2 + 1) * HD] = keys
                kv_out[seq, :, (head * 2 + 1) * HD : (head * 2 + 2) * HD] = values
            if has_past:
                before = past[seq, :, kv_span(head)]
                keys = jnp.concatenate((before[:, :HD], keys), axis=0)
                values = jnp.concatenate((before[:, HD:], values), axis=0)
            scores = lax.dot_general(
                queries, keys, (((1,), (1,)), ((), ())), preferred_element_type=jnp.float32
            )
            scores = jnp.where(causal, scores * scale, -1e30)
            highest = jnp.max(scores, axis=-1, keepdims=True)
            exponent = jnp.exp(scores - highest)
            total_weight = jnp.sum(exponent, axis=-1, keepdims=True)
            probabilities = (exponent / total_weight).astype(jnp.bfloat16)
            mixed = jnp.dot(probabilities, values, preferred_element_type=jnp.float32)
            mixed = mixed.astype(jnp.bfloat16)
            for h in range(group):
                column = (head * group + h) * HD
                mixed_all[span, column : column + HD] = mixed[h * tokens : (h + 1) * tokens, :]

    for n in range(OUT_STEPS):
        ready("o", n)
        out = jnp.dot(mixed_all[...], wo[:, out_span(n)], preferred_element_type=jnp.float32)
        for piece, ref in enumerate(outs):
            for seq in range(seqs):
                base = piece * rows + seq * tokens
                ref[seq, :, out_span(n)] = out[base : base + tokens].astype(ref.dtype)


def block(hidden, weights, tables, past, first, load):
    gain, wq, wkv, wo = weights
    pieces = len(hidden)
    seqs, tokens, width = hidden[0].shape
    rows = pieces * seqs * tokens
    kv_heads = wkv.shape[1] // (2 * HD)
    group = wq.shape[1] // HD // kv_heads
    cosine, sine = (table[first : first + tokens] for table in tables)
    vmem = pl.BlockSpec(memory_space=pltpu.VMEM)
    source = pl.BlockSpec(memory_space=pl.ANY) if load else vmem
    held = pltpu.HBM if load else pltpu.VMEM
    wq, wkv, wo = (pltpu.with_memory_space_constraint(w, held) for w in (wq, wkv, wo))
    if load:
        gain = pltpu.with_memory_space_constraint(gain, held)
        hidden = [pltpu.with_memory_space_constraint(hidden[0], held), *hidden[1:]]
    operands = [*hidden, gain, wq, wkv, wo, cosine, sine]
    in_specs = [source] * (pieces + 4) + [vmem, vmem]
    if load:
        for at in (0, *range(pieces, pieces + 4)):
            in_specs[at] = pl.BlockSpec(memory_space=pltpu.HBM)
    if past is not None:
        operands.append(past)
        in_specs.append(vmem)
    out_shape = [
        jax.ShapeDtypeStruct(
            (seqs, tokens, wo.shape[1]), jnp.bfloat16 if piece % 2 else jnp.float32
        )
        for piece in range(pieces)
    ]
    scratch = [
        pltpu.VMEM((rows, width), jnp.bfloat16),
        pltpu.VMEM((kv_heads, rows, group * HD), jnp.float32),
        pltpu.VMEM((kv_heads, rows, 2 * HD), jnp.float32),
        pltpu.VMEM((rows, wq.shape[1]), jnp.bfloat16),
    ]
    if load:
        out_shape += [pltpu.VMEM(w.shape, w.dtype) for w in (wq, wkv, wo)]
        scratch += [
            pltpu.VMEM((pieces, seqs, tokens, width), hidden[0].dtype),
            pltpu.VMEM(gain.shape, gain.dtype),
            pltpu.SemaphoreType.DMA((1 + pieces + 2 * kv_heads * K_STEPS + OUT_STEPS,)),
        ]
    else:
        out_shape += [jax.ShapeDtypeStruct((pieces * seqs, tokens, wkv.shape[1]), jnp.bfloat16)]
    kernel = functools.partial(
        block_kernel,
        pieces=pieces,
        load=load,
        has_past=past is not None,
        first=first,
        kv_heads=kv_heads,
        group=group,
    )
    flops = 2 * rows * width * (wq.shape[1] + wkv.shape[1] + wo.shape[0])
    result = pl.pallas_call(
        kernel,
        in_specs=in_specs,
        out_specs=[vmem] * len(out_shape),
        out_shape=out_shape,
        scratch_shapes=scratch,
        compiler_params=pltpu.CompilerParams(vmem_limit_bytes=VMEM_LIMIT),
        cost_estimate=pl.CostEstimate(
            flops=flops,
            transcendentals=0,
            bytes_accessed=2 * (wq.size + wkv.size + wo.size),
        ),
    )(*operands)
    return result[:pieces], result[pieces:]


def finish_kernel(*refs):
    *addends, _, out = refs
    total = addends[0][...]
    for ref in addends[1:]:
        total = total + ref[...].astype(jnp.float32)
    out[...] = total.astype(jnp.bfloat16)


def finish(own, whole_came, came, previous, c, chunk):
    seqs, _, width = own.shape
    column = width // 2
    ranged = pl.BlockSpec((seqs, chunk, column), lambda i: (0, c, i))
    single = pl.BlockSpec((seqs, chunk, column), lambda i: (0, 0, i))
    addends = [own, *whole_came, *came]
    specs = [ranged] * (1 + len(whole_came)) + [single] * len(came)
    aliases = {}
    if previous is None:
        previous = jnp.zeros((8, 128), jnp.bfloat16)
    else:
        aliases = {len(addends): 0}
    return pl.pallas_call(
        finish_kernel,
        grid=(width // column,),
        in_specs=specs + [pl.BlockSpec(memory_space=pl.ANY)],
        out_specs=ranged,
        out_shape=jax.ShapeDtypeStruct(own.shape, jnp.bfloat16),
        input_output_aliases=aliases,
        compiler_params=pltpu.CompilerParams(
            dimension_semantics=("arbitrary",), vmem_limit_bytes=16 * 2**20
        ),
    )(*addends, previous)


def join_heads(kv_weight):
    sharers = max(lax.axis_size("tensor") // KVH, 1)
    position = lax.axis_index("tensor")
    for bit_index in range(sharers.bit_length() - 1):
        bit = 1 << bit_index
        partner = hop(kv_weight, bit)
        keeps_first = position // bit % 2 == 0
        kv_weight = jnp.concatenate(
            (
                jnp.where(keeps_first, kv_weight, partner),
                jnp.where(keeps_first, partner, kv_weight),
            ),
            axis=1,
        )
    return kv_weight


def layer(hidden_in, norm_gain, query_weight, kv_weight, output_weight):
    parts = lax.axis_size("tensor")
    _, length, width = hidden_in.shape
    tables = rotary_tables(length)
    weights = (norm_gain.reshape(1, width), query_weight, join_heads(kv_weight), output_weight)
    near = [m for m in range(parts) if m < 2]
    far = [m for m in range(parts) if m >= 2]
    groups = [far[i : i + 2] for i in range(0, len(far), 2)]
    chunk = length // CHUNKS
    spans = [slice(c * chunk, (c + 1) * chunk) for c in range(CHUNKS)]

    arrived = {0: hidden_in}
    if len(near) > 1:
        arrived[1] = hop(hidden_in, 1)
    far_arrived = []
    for span in spans:
        held = {0: hidden_in[:, span]}
        for m in far:
            low = m & -m
            if m ^ low == 1:
                held[1] = arrived[1][:, span]
            held[m] = hop(held[m ^ low], low)
        far_arrived.append(held)

    near_out, held_weights = block([arrived[m] for m in near], weights, tables, None, 0, True)
    weights = (weights[0], *held_weights)
    own = near_out[0]
    near_came = []
    if len(near) > 1:
        near_came = [hop(near_out[1], 1)]

    pasts = [None for _ in groups]
    result = None
    for c in range(CHUNKS):
        totals = {}
        for g, group in enumerate(groups):
            out, (kv,) = block(
                [far_arrived[c][m] for m in group], weights, tables, pasts[g], c * chunk, False
            )
            pasts[g] = kv if pasts[g] is None else jnp.concatenate((pasts[g], kv), axis=1)
            totals.update(zip(group, out))
        came = []
        for m in reversed(far):
            low = m & -m
            back = hop(totals[m].astype(jnp.bfloat16), low)
            if m ^ low:
                totals[m ^ low] = totals[m ^ low] + back.astype(jnp.float32)
            else:
                came.append(back)
        result = finish(own, near_came, came, result, c, chunk)
    return result


def solution(mesh):
    placed = (
        P(("dp", "tensor"), None, None),
        P(),
        P(None, "tensor"),
        P(None, "tensor"),
        P("tensor", None),
    )
    return jax.shard_map(
        layer,
        mesh=mesh,
        in_specs=placed,
        out_specs=P(("dp", "tensor"), None, None),
        check_vma=False,
    )
```

```python
import functools
import math

import jax
import jax.numpy as jnp
from jax import lax
from jax.experimental import pallas as pl
from jax.experimental.pallas import tpu as pltpu
from jax.sharding import PartitionSpec as P


KVH = 8
HD = 128

EPS = 1e-05
THETA = 500000.0

CHUNKS = 2
K_STEPS = 4
OUT_STEPS = 4
VMEM_LIMIT = 12 * 2**20


def hop(value, bit):
    pairs = [(source, source ^ bit) for source in range(lax.axis_size("tensor"))]
    return lax.ppermute(value, "tensor", pairs)


def rotary_tables(length):
    half_width = HD // 2
    frequency = THETA ** (-(jnp.arange(half_width, dtype=jnp.float32) * 2.0 / HD))
    angles = jnp.arange(length, dtype=jnp.float32)[:, None] * frequency[None, :]
    cosine = jnp.cos(angles)
    sine = jnp.sin(angles)
    return (
        jnp.concatenate((cosine, cosine), axis=1),
        jnp.concatenate((-sine, sine), axis=1),
    )


def block_kernel(*refs, pieces, load, has_past, first, kv_heads, group):
    hidden = list(refs[:pieces])
    gain, wq, wkv, wo, cosine_ref, sine_ref = refs[pieces : pieces + 6]
    at = pieces + 6
    past = refs[at] if has_past else None
    at += has_past
    outs = refs[at : at + pieces]
    at += pieces
    copies = {}
    if load:
        wq_to, wkv_to, wo_to, normed, q_acc, kv_acc, mixed_all, held, gain_to, sems = refs[at:]
        k_steps = K_STEPS
    else:
        kv_out, normed, q_acc, kv_acc, mixed_all = refs[at:]
        k_steps = 1
    seqs, tokens, width = hidden[0].shape
    rows = seqs * tokens
    k_block = width // k_steps
    out_block = wo.shape[1] // OUT_STEPS

    def k_span(k):
        return slice(k * k_block, (k + 1) * k_block)

    def q_span(head):
        return slice(head * group * HD, (head + 1) * group * HD)

    def kv_span(head):
        return slice(head * 2 * HD, (head + 1) * 2 * HD)

    def out_span(n):
        return slice(n * out_block, (n + 1) * out_block)

    if load:

        def start(name, source, target):
            copy = pltpu.make_async_copy(source, target, sems.at[len(copies)])
            copy.start()
            copies[name] = copy

        start("gain", gain, gain_to)
        for piece, ref in enumerate(hidden):
            start(("x", piece), ref, held.at[piece])
            hidden[piece] = held.at[piece]
        for head in range(kv_heads):
            for k in range(k_steps):
                source = (k_span(k), q_span(head))
                start(("q", head, k), wq.at[source], wq_to.at[source])
                source = (k_span(k), kv_span(head))
                start(("kv", head, k), wkv.at[source], wkv_to.at[source])
        for n in range(OUT_STEPS):
            source = (slice(None), out_span(n))
            start(("o", n), wo.at[source], wo_to.at[source])
        gain, wq, wkv, wo = gain_to, wq_to, wkv_to, wo_to

    def ready(*name):
        if load:
            copies[name if len(name) > 1 else name[0]].wait()

    ready("gain")
    for piece, ref in enumerate(hidden):
        ready("x", piece)
        for seq in range(seqs):
            wide = ref[seq].astype(jnp.float32)
            mean_square = jnp.mean(wide * wide, axis=-1, keepdims=True)
            result = (wide * lax.rsqrt(mean_square + EPS) * gain[...]).astype(jnp.bfloat16)
            base = piece * rows + seq * tokens
            normed[base : base + tokens, :] = result

    cosine = cosine_ref[...]
    sine = sine_ref[...]

    def rotate(value):
        return (value * cosine + pltpu.roll(value, HD // 2, 1) * sine).astype(jnp.bfloat16)

    scale = 1.0 / math.sqrt(HD)
    total = first + tokens
    query_at = lax.broadcasted_iota(jnp.int32, (tokens, total), 0) + first
    key_at = lax.broadcasted_iota(jnp.int32, (tokens, total), 1)
    causal = jnp.concatenate([query_at - key_at] * group, axis=0) >= 0

    for head in range(kv_heads):
        for k in range(k_steps):
            ready("q", head, k)
            ready("kv", head, k)
            x = normed[:, k_span(k)]
            q_part = jnp.dot(x, wq[k_span(k), q_span(head)], preferred_element_type=jnp.float32)
            kv_part = jnp.dot(x, wkv[k_span(k), kv_span(head)], preferred_element_type=jnp.float32)
            if k == 0:
                q_acc[head] = q_part
                kv_acc[head] = kv_part
            else:
                q_acc[head] += q_part
                kv_acc[head] += kv_part
        for seq in range(pieces * seqs):
            span = slice(seq * tokens, (seq + 1) * tokens)
            queries = jnp.concatenate(
                [rotate(q_acc[head, span, h * HD : (h + 1) * HD]) for h in range(group)], axis=0
            )
            raw = kv_acc[head, span, :].astype(jnp.bfloat16)
            keys = rotate(raw[:, :HD].astype(jnp.float32))
            values = raw[:, HD:]
            if not load:
                kv_out[seq, :, head * 2 * HD : (head * 2 + 1) * HD] = keys
                kv_out[seq, :, (head * 2 + 1) * HD : (head * 2 + 2) * HD] = values
            if has_past:
                before = past[seq, :, kv_span(head)]
                keys = jnp.concatenate((before[:, :HD], keys), axis=0)
                values = jnp.concatenate((before[:, HD:], values), axis=0)
            scores = lax.dot_general(
                queries, keys, (((1,), (1,)), ((), ())), preferred_element_type=jnp.float32
            )
            scores = jnp.where(causal, scores * scale, -1e30)
            highest = jnp.max(scores, axis=-1, keepdims=True)
            exponent = jnp.exp(scores - highest)
            total_weight = jnp.sum(exponent, axis=-1, keepdims=True)
            probabilities = (exponent / total_weight).astype(jnp.bfloat16)
            mixed = jnp.dot(probabilities, values, preferred_element_type=jnp.float32)
            mixed = mixed.astype(jnp.bfloat16)
            for h in range(group):
                column = (head * group + h) * HD
                mixed_all[span, column : column + HD] = mixed[h * tokens : (h + 1) * tokens, :]

    for n in range(OUT_STEPS):
        ready("o", n)
        out = jnp.dot(mixed_all[...], wo[:, out_span(n)], preferred_element_type=jnp.float32)
        for piece, ref in enumerate(outs):
            for seq in range(seqs):
                base = piece * rows + seq * tokens
                ref[seq, :, out_span(n)] = out[base : base + tokens].astype(ref.dtype)


def block(hidden, weights, tables, past, first, load):
    gain, wq, wkv, wo = weights
    pieces = len(hidden)
    seqs, tokens, width = hidden[0].shape
    rows = pieces * seqs * tokens
    kv_heads = wkv.shape[1] // (2 * HD)
    group = wq.shape[1] // HD // kv_heads
    cosine, sine = (table[first : first + tokens] for table in tables)
    vmem = pl.BlockSpec(memory_space=pltpu.VMEM)
    source = pl.BlockSpec(memory_space=pl.ANY) if load else vmem
    held = pltpu.HBM if load else pltpu.VMEM
    wq, wkv, wo = (pltpu.with_memory_space_constraint(w, held) for w in (wq, wkv, wo))
    if load:
        gain = pltpu.with_memory_space_constraint(gain, held)
        hidden = [pltpu.with_memory_space_constraint(hidden[0], held), *hidden[1:]]
    operands = [*hidden, gain, wq, wkv, wo, cosine, sine]
    in_specs = [source] * (pieces + 4) + [vmem, vmem]
    if load:
        for at in (0, *range(pieces, pieces + 4)):
            in_specs[at] = pl.BlockSpec(memory_space=pltpu.HBM)
    if past is not None:
        operands.append(past)
        in_specs.append(vmem)
    out_shape = [
        jax.ShapeDtypeStruct(
            (seqs, tokens, wo.shape[1]), jnp.bfloat16 if piece % 2 else jnp.float32
        )
        for piece in range(pieces)
    ]
    scratch = [
        pltpu.VMEM((rows, width), jnp.bfloat16),
        pltpu.VMEM((kv_heads, rows, group * HD), jnp.float32),
        pltpu.VMEM((kv_heads, rows, 2 * HD), jnp.float32),
        pltpu.VMEM((rows, wq.shape[1]), jnp.bfloat16),
    ]
    if load:
        out_shape += [pltpu.VMEM(w.shape, w.dtype) for w in (wq, wkv, wo)]
        scratch += [
            pltpu.VMEM((pieces, seqs, tokens, width), hidden[0].dtype),
            pltpu.VMEM(gain.shape, gain.dtype),
            pltpu.SemaphoreType.DMA((1 + pieces + 2 * kv_heads * K_STEPS + OUT_STEPS,)),
        ]
    else:
        out_shape += [jax.ShapeDtypeStruct((pieces * seqs, tokens, wkv.shape[1]), jnp.bfloat16)]
    kernel = functools.partial(
        block_kernel,
        pieces=pieces,
        load=load,
        has_past=past is not None,
        first=first,
        kv_heads=kv_heads,
        group=group,
    )
    flops = 2 * rows * width * (wq.shape[1] + wkv.shape[1] + wo.shape[0])
    result = pl.pallas_call(
        kernel,
        in_specs=in_specs,
        out_specs=[vmem] * len(out_shape),
        out_shape=out_shape,
        scratch_shapes=scratch,
        compiler_params=pltpu.CompilerParams(vmem_limit_bytes=VMEM_LIMIT),
        cost_estimate=pl.CostEstimate(
            flops=flops,
            transcendentals=0,
            bytes_accessed=2 * (wq.size + wkv.size + wo.size),
        ),
    )(*operands)
    return result[:pieces], result[pieces:]


def finish_kernel(*refs, c, near, aliased):
    own, *addends = refs[: len(refs) - 3 - aliased]
    out, total_held, sems = refs[-3:]
    _, chunk, width = total_held.shape
    span = slice(c * chunk, (c + 1) * chunk)
    parts = 2
    copies = []
    for part in range(parts):
        columns = slice(part * width // parts, (part + 1) * width // parts)
        total = own[:, span, columns]
        for at, ref in enumerate(addends):
            rows = span if at < near else slice(None)
            total = total + ref[:, rows, columns].astype(jnp.float32)
        total_held[:, :, columns] = total.astype(jnp.bfloat16)
        copies.append(
            pltpu.make_async_copy(
                total_held.at[:, :, columns], out.at[:, span, columns], sems.at[part]
            )
        )
        copies[-1].start()
    for copy in copies:
        copy.wait()


def finish(own, whole_came, came, previous, c, chunk):
    seqs, _, width = own.shape
    vmem = pl.BlockSpec(memory_space=pltpu.VMEM)
    hbm = pl.BlockSpec(memory_space=pltpu.HBM)
    operands = [own, *whole_came, *came]
    specs = [vmem] * len(operands)
    aliases = {}
    if previous is not None:
        aliases = {len(operands): 0}
        operands.append(previous)
        specs.append(hbm)
    return pl.pallas_call(
        functools.partial(
            finish_kernel, c=c, near=len(whole_came), aliased=int(previous is not None)
        ),
        in_specs=specs,
        out_specs=hbm,
        out_shape=pltpu.HBM(own.shape, jnp.bfloat16),
        scratch_shapes=[
            pltpu.VMEM((seqs, chunk, width), jnp.bfloat16),
            pltpu.SemaphoreType.DMA((2,)),
        ],
        input_output_aliases=aliases,
        compiler_params=pltpu.CompilerParams(vmem_limit_bytes=VMEM_LIMIT),
    )(*operands)


def join_heads(kv_weight):
    sharers = max(lax.axis_size("tensor") // KVH, 1)
    position = lax.axis_index("tensor")
    for bit_index in range(sharers.bit_length() - 1):
        bit = 1 << bit_index
        partner = hop(kv_weight, bit)
        keeps_first = position // bit % 2 == 0
        kv_weight = jnp.concatenate(
            (
                jnp.where(keeps_first, kv_weight, partner),
                jnp.where(keeps_first, partner, kv_weight),
            ),
            axis=1,
        )
    return kv_weight


def layer(hidden_in, norm_gain, query_weight, kv_weight, output_weight):
    parts = lax.axis_size("tensor")
    _, length, width = hidden_in.shape
    tables = rotary_tables(length)
    weights = (norm_gain.reshape(1, width), query_weight, join_heads(kv_weight), output_weight)
    near = [m for m in range(parts) if m < 2]
    far = [m for m in range(parts) if m >= 2]
    groups = [far[i : i + 2] for i in range(0, len(far), 2)]
    chunk = length // CHUNKS
    spans = [slice(c * chunk, (c + 1) * chunk) for c in range(CHUNKS)]

    arrived = {0: hidden_in}
    if len(near) > 1:
        arrived[1] = hop(hidden_in, 1)
    far_arrived = []
    later = hidden_in
    for span in spans:
        part, later = lax.optimization_barrier((later[:, span], later))
        held = {0: part}
        for m in far:
            low = m & -m
            if m ^ low == 1:
                held[1] = arrived[1][:, span]
            held[m] = hop(held[m ^ low], low)
        far_arrived.append(held)

    near_out, held_weights = block([arrived[m] for m in near], weights, tables, None, 0, True)
    weights = (weights[0], *held_weights)
    own = near_out[0]
    near_came = []
    if len(near) > 1:
        near_came = [hop(near_out[1], 1)]

    pasts = [None for _ in groups]
    result = None
    for c in range(CHUNKS):
        totals = {}
        for g, group in enumerate(groups):
            out, (kv,) = block(
                [far_arrived[c][m] for m in group], weights, tables, pasts[g], c * chunk, False
            )
            pasts[g] = kv if pasts[g] is None else jnp.concatenate((pasts[g], kv), axis=1)
            totals.update(zip(group, out))
        came = []
        for m in reversed(far):
            low = m & -m
            back = hop(totals[m].astype(jnp.bfloat16), low)
            if m ^ low:
                totals[m ^ low] = totals[m ^ low] + back.astype(jnp.float32)
            else:
                came.append(back)
        result = finish(own, near_came, came, result, c, chunk)
    return result


def solution(mesh):
    placed = (
        P(("dp", "tensor"), None, None),
        P(),
        P(None, "tensor"),
        P(None, "tensor"),
        P("tensor", None),
    )
    return jax.shard_map(
        layer,
        mesh=mesh,
        in_specs=placed,
        out_specs=P(("dp", "tensor"), None, None),
        check_vma=False,
    )
```
